32 devices in a mesh: expert: 2 (over x), dp: 16 (over z, y, core).
Axes of the slice: x: 2, y: 2, z: 4, core: 2. Of those that a mesh axis runs over, the one named last changes fastest.
Arguments:
- tokens: bfloat16 [256, 4096], P(('expert', 'dp')), may hold values from -6 to 6
- expert_ids: int32 [256, 2], P(('expert', 'dp')), may hold values from 0 to 1, as said below
- slots: int32 [256, 2], P(('expert', 'dp')), may hold values from -1 to 1, as said below
- mix_weights: float32 [256, 2], P(('expert', 'dp')), may hold values from 0.1 to 1
- w_gate: bfloat16 [2, 4096, 8192], P('expert', None, 'dp'), may hold values from -0.09375 to 0.09375
- w_up: bfloat16 [2, 4096, 8192], P('expert', None, 'dp'), may hold values from -0.09375 to 0.09375
- w_down: bfloat16 [2, 8192, 4096], P('expert', None, 'dp'), may hold values from -0.0625 to 0.0625
Outputs:
- mixed: bfloat16 [256, 4096], P(('expert', 'dp'))
The draws below stay inside these ranges and needn't reach their ends.
Inputs may be any that keep to these rules, and one draw needn't show every extreme that they name: `expert_ids`: each token names 2 different experts. Within each aligned block of 8 tokens (the tokens of one device), the assignments to one expert get distinct slots among 0 to 1 in some order, at most 2 of them are kept and the others get -1; an expert with 2 or more assignments in the block has all 2 slots used. No two assignments of one block share an expert and a slot. In every block some expert has all 2 slots used.
All inputs are finite; a program needn't handle non-finite values.
Results may differ from the reference program's by a relative error of at most 0.0085.
Values may be sent and summed in bfloat16 or wider, within the bound.
A program may use at most 128 MiB of HBM per device.

```python
import jax
import jax.numpy as jnp
from jax import lax

D = 4096
FFW = 8192
TOP = 2
TOK_DEV = 8
CAP = 2
EXPERTS = 2
TOKENS = 256
N_DP = 16


def routing(key):
    folded = jax.random.fold_in(key, 17)
    jitter_key, lean_key, favour_key, order_key = jax.random.split(folded, 4)
    jitter = jax.random.randint(jitter_key, (TOKENS, EXPERTS), 0, 2 ** 20)
    lean_bias = jax.random.randint(lean_key, (EXPERTS,), 0, 4) * 2 ** 19
    favoured = jax.random.randint(favour_key, (N_DP,), 0, EXPERTS)
    block_id = jnp.arange(TOKENS, dtype=jnp.int32) // TOK_DEV
    position = jnp.arange(TOKENS, dtype=jnp.int32) % TOK_DEV
    favoured_tok = favoured[block_id % N_DP]
    expert_line = jnp.arange(EXPERTS, dtype=jnp.int32)
    booster = ((position < CAP)[:, None] & (expert_line[None, :] == favoured_tok[:, None])).astype(jnp.int32) * 2 ** 23
    scores = (jitter + lean_bias[None, :] + booster) * EXPERTS + expert_line[None, :]
    top_scores, chosen = lax.top_k(scores, TOP)
    chosen = chosen.astype(jnp.int32)
    grouped = chosen.reshape(TOKENS // TOK_DEV, TOK_DEV * TOP)
    same_expert = grouped[:, :, None] == grouped[:, None, :]
    order_line = jnp.arange(TOK_DEV * TOP, dtype=jnp.int32)
    priority = jax.random.randint(order_key, (TOKENS // TOK_DEV, TOK_DEV * TOP), 0, 2 ** 16) * (TOK_DEV * TOP) + order_line[None, :]
    earlier = priority[:, None, :] < priority[:, :, None]
    position_rank = jnp.sum((same_expert & earlier).astype(jnp.int32), axis=2)
    slot_values = jnp.where(position_rank < CAP, position_rank, -1).astype(jnp.int32)
    return (chosen, slot_values.reshape(TOKENS, TOP))


def draw_expert_ids(key, part):
    return routing(key)[0]


def draw_slots(key, part):
    return routing(key)[1]


def levels(own_key, extent, cuts, least, largest):
    factor_of = 1.0
    for dim, parts in cuts:
        heights = jax.random.uniform(jax.random.fold_in(jax.random.fold_in(own_key, 6), dim), (parts,), jnp.float32, least / len(cuts), largest / len(cuts))
        factor_of = factor_of * jnp.repeat(jnp.exp(heights), extent[dim] // parts).reshape((-1,) + (1,) * (len(extent) - 1 - dim))
    return factor_of


def noise(own_key, shape, scale, most, cuts=(), held_as=jnp.bfloat16):
    level = levels(own_key, shape, cuts, -0.22, 0.18) if cuts else 1.0
    values = jax.random.normal(own_key, shape, jnp.float32) * scale * level
    return jnp.minimum(jnp.maximum(values, -most), most).astype(held_as)


def setup_inputs(seed: int = 0) -> dict:
    splits = jax.random.split(jax.random.key(seed), 8)
    tokens = noise(splits[0], (TOKENS, D), 1.0, 6.0, ((0, 32),))
    expert_ids = draw_expert_ids(jax.random.fold_in(splits[7], 71), 0)
    slots = draw_slots(jax.random.fold_in(splits[7], 71), 0)
    mix_weights = jnp.clip(0.1 + 0.9 * jax.random.uniform(splits[3], (TOKENS, TOP), jnp.float32) ** levels(splits[3], (TOKENS, TOP), ((0, 32),), -0.2, 0.2), 0.1, 1.0)
    w_gate = noise(splits[4], (EXPERTS, D, FFW), D ** -0.5, 0.09375, ((0, 2), (2, 16)))
    w_up = noise(splits[5], (EXPERTS, D, FFW), D ** -0.5, 0.09375, ((0, 2), (2, 16)))
    w_down = noise(splits[6], (EXPERTS, FFW, D), FFW ** -0.5, 0.0625, ((0, 2), (2, 16)))
    return dict(tokens=tokens, expert_ids=expert_ids, slots=slots, mix_weights=mix_weights, w_gate=w_gate, w_up=w_up, w_down=w_down)


def reference(tokens, expert_ids, slots, mix_weights, w_gate, w_up, w_down):
    block_count = TOKENS // TOK_DEV
    block_of = jnp.arange(TOKENS, dtype=jnp.int32) // TOK_DEV
    block_idx = jnp.broadcast_to(block_of[:, None], (TOKENS, TOP)).astype(jnp.int32)
    is_kept = slots >= 0
    slot_place = jnp.where(is_kept, slots, CAP).astype(jnp.int32)
    spread = jnp.broadcast_to(tokens[:, None, :], (TOKENS, TOP, D))
    buffer = jnp.zeros((EXPERTS, block_count, CAP, D), jnp.bfloat16)
    buffer = buffer.at[expert_ids, block_idx, slot_place].set(spread, mode="drop")

    def expert_ffn(operands):
        slab, gate_w, up_w, down_w = operands
        flattened = slab.reshape(block_count * CAP, D)
        gate_part = jnp.dot(flattened, gate_w, preferred_element_type=jnp.float32)
        up_part = jnp.dot(flattened, up_w, preferred_element_type=jnp.float32)
        hidden = (jax.nn.silu(gate_part) * up_part).astype(jnp.bfloat16)
        result = jnp.dot(hidden, down_w, preferred_element_type=jnp.float32).astype(jnp.bfloat16)
        return result.reshape(block_count, CAP, D)

    outputs = lax.map(expert_ffn, (buffer, w_gate, w_up, w_down))
    picked = outputs[expert_ids, block_idx, jnp.minimum(slot_place, CAP - 1)]
    weighted = jnp.where(is_kept[:, :, None], mix_weights[:, :, None] * picked.astype(jnp.float32), 0.0)
    return jnp.sum(weighted, axis=1).astype(jnp.bfloat16)
```

```python
import functools

import jax
import jax.numpy as jnp
from jax import lax
from jax.experimental import pallas as pl
from jax.experimental.pallas import tpu as pltpu
from jax.sharding import PartitionSpec as P

CAP = 2
PLANE = 4
HALVES = 2
BF = jnp.bfloat16
F32 = jnp.float32


def collective_form(tokens, expert_ids, slots, mix_weights, w_gate, w_up, w_down):
    tok_rows, model_width = tokens.shape
    experts = lax.axis_size("expert")
    slot_count = experts * CAP
    slot_ids = jnp.arange(slot_count, dtype=jnp.int32)
    matches = (expert_ids[None, :, :] == (slot_ids // CAP)[:, None, None]) & (
        slots[None, :, :] == (slot_ids % CAP)[:, None, None]
    )
    table = jnp.any(matches, axis=2).astype(BF)
    outgoing = jnp.dot(table, tokens, preferred_element_type=F32).astype(BF)
    arrived = lax.all_to_all(outgoing, "expert", split_axis=0, concat_axis=0, tiled=True)
    portion = lax.all_gather(arrived, "dp", axis=0, tiled=True)
    gate_part = jnp.dot(portion, w_gate[0], preferred_element_type=F32)
    up_part = jnp.dot(portion, w_up[0], preferred_element_type=F32)
    hidden = (jax.nn.silu(gate_part) * up_part).astype(BF)
    summed = jnp.dot(
        lax.all_gather(hidden, "dp", axis=1, tiled=True), w_down[0], preferred_element_type=F32
    )
    result = summed.astype(BF)
    blocks = result.reshape(lax.axis_size("dp"), experts, CAP, result.shape[1])
    blocks = lax.all_to_all(blocks, "expert", split_axis=1, concat_axis=1, tiled=True)
    blocks = lax.all_to_all(blocks, "dp", split_axis=0, concat_axis=3, tiled=True)
    returned = blocks.reshape(slot_count, model_width)
    weight_table = jnp.sum(jnp.where(matches, mix_weights[None, :, :], 0.0), axis=2)
    mixed = jnp.dot(
        weight_table.T,
        returned.astype(F32),
        precision=lax.Precision.HIGHEST,
        preferred_element_type=F32,
    )
    return mixed.astype(BF)


def kernel(
    experts, groups,
    tok_ref, ids_ref, slot_ref, mix_ref, wg_hbm, wu_hbm, wd_hbm, out_ref,
    wg, wu, wd, obuf, ubuf, xbuf, hbuf, pbuf, rbuf,
    wsem, s1s, s1r, s2s, s2r, s3s, s3r, azs, azr, ays, ayr, acs, acr, rs, rr,
):
    planes = groups // PLANE
    units = experts * planes
    rows = units * CAP
    tok_rows, width = tok_ref.shape
    half = width // HALVES
    chunk_count = rows // CAP
    chunk = half // chunk_count
    cols = wd.shape[2]
    x = lax.axis_index("expert")
    d = lax.axis_index("dp")
    z, b = d // PLANE, d % PLANE
    y, c = b // 2, b % 2
    unit = x * planes + z
    y_block = (1 - y) * 2 + c
    c_block = y * 2 + 1 - c
    yc_block = (1 - y) * 2 + 1 - c

    def dev(xx, dd):
        return (xx, dd)

    def rdma(src, dst, ssem, rsem, device):
        return pltpu.make_async_remote_copy(
            src_ref=src, dst_ref=dst, send_sem=ssem, recv_sem=rsem,
            device_id=device, device_id_type=pl.DeviceIdType.MESH,
        )

    y_dev = dev(x, z * PLANE + y_block)
    c_dev = dev(x, z * PLANE + c_block)
    offsets = [(dx, dz) for dz in range(planes) for dx in range(experts) if dx or dz]

    def peer(dx, dz):
        return lax.rem(x + dx, experts), lax.rem(z + dz, planes)

    barrier = pltpu.get_barrier_semaphore()
    for dx, dz in offsets:
        px, pz = peer(dx, dz)
        pl.semaphore_signal(barrier, inc=1, device_id=dev(px, pz * PLANE + b),
                            device_id_type=pl.DeviceIdType.MESH)
    for other in (y_dev, c_dev):
        pl.semaphore_signal(barrier, inc=1, device_id=other,
                            device_id_type=pl.DeviceIdType.MESH)

    loads = []
    for h in range(HALVES):
        part = pl.ds(h * half, half)
        loads.append(pltpu.make_async_copy(wg_hbm.at[0, part], wg.at[part], wsem.at[2 * h]))
        loads.append(pltpu.make_async_copy(wu_hbm.at[0, part], wu.at[part], wsem.at[2 * h + 1]))
    depth = wd.shape[1]
    for g in range(groups):
        loads.append(pltpu.make_async_copy(
            wd_hbm.at[0, pl.ds(g * depth, depth)], wd.at[g], wsem.at[2 * HALVES + g]))
    for load in loads:
        load.start()

    ids = ids_ref[...]
    places = slot_ref[...]
    lanes = experts * chunk_count * CAP
    lane = lax.broadcasted_iota(jnp.int32, (tok_rows, 128), 1)
    lane_e, lane_r = lane // (chunk_count * CAP), lane % CAP
    hit = jnp.zeros((tok_rows, 128), F32)
    for k in range(ids.shape[1]):
        same = (ids[:, k:k + 1] == lane_e) & (places[:, k:k + 1] == lane_r)
        hit = jnp.where(same, 1.0, hit)
    tall = jnp.concatenate([hit] * chunk_count, axis=0)
    tall_row = lax.broadcasted_iota(jnp.int32, tall.shape, 0) // tok_rows
    tall_lane = (lax.broadcasted_iota(jnp.int32, tall.shape, 1) // CAP) % chunk_count
    pick = jnp.where(tall_row == tall_lane, tall, 0.0).T[:lanes].astype(BF)
    for h in range(HALVES):
        stack = jnp.concatenate(
            [tok_ref[:, h * half + j * chunk: h * half + (j + 1) * chunk].astype(F32)
             for j in range(chunk_count)], axis=0).astype(BF)
        sent = jnp.dot(pick, stack, preferred_element_type=F32).astype(BF)
        for e in range(experts):
            obuf[h, e] = sent[e * rows:(e + 1) * rows]
    weight_cols = {}
    mix = mix_ref[...]
    for e in range(experts):
        for r in range(CAP):
            total = jnp.zeros((tok_rows, 1), F32)
            for k in range(ids.shape[1]):
                total += jnp.where((ids[:, k:k + 1] == e) & (places[:, k:k + 1] == r),
                                   mix[:, k:k + 1], 0.0)
            weight_cols[e, r] = total

    pl.semaphore_wait(barrier, len(offsets) + 2)

    waits = []
    for h in range(HALVES):
        for n, (dx, dz) in reversed(list(enumerate(offsets))):
            px, pz = peer(dx, dz)
            copy = rdma(obuf.at[h, px], ubuf.at[h, unit], s1s.at[h, n], s1r.at[h, unit],
                        dev(px, pz * PLANE + b))
            copy.start()
            waits.append(copy)
    for h in range(HALVES):
        ubuf[h, unit] = obuf[h, x]

    count = units * chunk_count * CAP
    pr = lax.broadcasted_iota(jnp.int32, (count, count), 0)
    pc = lax.broadcasted_iota(jnp.int32, (count, count), 1)
    source = ((pr // CAP) % units) * (chunk_count * CAP) + (pr // rows) * CAP + pr % CAP
    order = jnp.where(pc == source, 1.0, 0.0).astype(BF)

    def arrival(buf, h, slot, rsem):
        return rdma(buf, buf, s2s.at[0], rsem, y_dev)

    gate = up = None
    for h in range(HALVES):
        for dx, dz in offsets:
            px, pz = peer(dx, dz)
            pu = px * planes + pz
            rdma(ubuf.at[h, pu], ubuf.at[h, pu], s1s.at[0, 0], s1r.at[h, pu], y_dev).wait_recv()
        arrived = ubuf[h].reshape(count, chunk)
        block = jnp.dot(order, arrived, preferred_element_type=F32).astype(BF)
        for j in range(chunk_count):
            xbuf[h, b, :, j * chunk:(j + 1) * chunk] = block[j * rows:(j + 1) * rows]
        mine = xbuf.at[h, b]
        to_y = rdma(mine, mine, s2s.at[h], s2r.at[h], y_dev)
        to_y.start()
        to_c = rdma(mine, mine, s3s.at[h, 0], s3r.at[h, 0], c_dev)
        to_c.start()
        waits += [to_y, to_c]
    for h in range(HALVES):
        theirs = xbuf.at[h, y_block]
        rdma(theirs, theirs, s2s.at[h], s2r.at[h], y_dev).wait_recv()
        forward = rdma(theirs, theirs, s3s.at[h, 1], s3r.at[h, 1], c_dev)
        forward.start()
        waits.append(forward)
        for n, blk in enumerate((c_block, yc_block)):
            got = xbuf.at[h, blk]
            rdma(got, got, s3s.at[h, n], s3r.at[h, n], c_dev).wait_recv()
        loads[2 * h].wait()
        loads[2 * h + 1].wait()
        part = pl.ds(h * half, half)
        slab = xbuf[h].reshape(PLANE * rows, half)
        g_part = jnp.dot(slab, wg[part], preferred_element_type=F32)
        u_part = jnp.dot(slab, wu[part], preferred_element_type=F32)
        gate = g_part if gate is None else gate + g_part
        up = u_part if up is None else up + u_part
    hidden = (gate / (1.0 + jnp.exp(-gate)) * up).astype(BF)
    hbuf[d] = hidden

    def dp_of(zz, blk):
        return zz * PLANE + blk

    shard = hbuf.at[d]
    for dz in range(planes - 1, 0, -1):
        pz = lax.rem(z + dz, planes)
        copy = rdma(shard, shard, azs.at[dz], azr.at[z], dev(x, dp_of(pz, b)))
        copy.start()
        waits.append(copy)
    copy = rdma(shard, shard, ays.at[0], ayr.at[z], y_dev)
    copy.start()
    waits.append(copy)
    copy = rdma(shard, shard, acs.at[0], acr.at[z, 0], c_dev)
    copy.start()
    waits.append(copy)
    for load in loads[2 * HALVES:]:
        load.wait()

    def product(g):
        return jnp.dot(hbuf[g], wd[g], preferred_element_type=F32)

    acc = product(d)
    for dz in range(planes):
        pz = lax.rem(z + dz, planes)
        if dz:
            g = dp_of(pz, b)
            got = hbuf.at[g]
            rdma(got, got, azs.at[dz], azr.at[pz], y_dev).wait_recv()
            on_y = rdma(got, got, ays.at[dz], ayr.at[pz], y_dev)
            on_y.start()
            on_c = rdma(got, got, acs.at[dz], acr.at[pz, 0], c_dev)
            on_c.start()
            waits += [on_y, on_c]
            acc += product(g)
        g = dp_of(pz, c_block)
        got = hbuf.at[g]
        rdma(got, got, acs.at[0], acr.at[pz, 0], c_dev).wait_recv()
        acc += product(g)
    for dz in range(planes):
        pz = lax.rem(z + dz, planes)
        g = dp_of(pz, y_block)
        got = hbuf.at[g]
        rdma(got, got, ays.at[0], ayr.at[pz], y_dev).wait_recv()
        on_c = rdma(got, got, acs.at[planes + dz], acr.at[pz, 1], c_dev)
        on_c.start()
        waits.append(on_c)
        acc += product(g)
    for dz in range(planes):
        pz = lax.rem(z + dz, planes)
        g = dp_of(pz, yc_block)
        got = hbuf.at[g]
        rdma(got, got, acs.at[0], acr.at[pz, 1], c_dev).wait_recv()
        acc += product(g)

    wide = cols // 128
    piece_rows = wide * CAP
    everyone = experts * groups
    result = acc.astype(BF)
    for w in range(wide):
        for p in range(everyone):
            pbuf[p, w * CAP:(w + 1) * CAP, :] = result[p * CAP:(p + 1) * CAP,
                                                       w * 128:(w + 1) * 128]
    me = x * groups + d

    def piece_of(device):
        dx, dd = device // groups, device % groups
        return (dd % PLANE) * units + dx * planes + dd // PLANE

    rbuf[me] = pbuf[piece_of(me)]
    for k in range(1, everyone):
        other = lax.rem(me + k, everyone)
        copy = rdma(pbuf.at[piece_of(other)], rbuf.at[me], rs.at[k], rr.at[me],
                    dev(other // groups, other % groups))
        copy.start()
        waits.append(copy)
    for k in range(1, everyone):
        other = lax.rem(me + k, everyone)
        rdma(rbuf.at[other], rbuf.at[other], rs.at[k], rr.at[other], y_dev).wait_recv()
    for g in range(groups):
        pieces = [rbuf[e * groups + g].astype(F32) for e in range(experts)]
        for w in range(wide):
            total = None
            for e in range(experts):
                for r in range(CAP):
                    term = weight_cols[e, r] * pieces[e][w * CAP + r:w * CAP + r + 1]
                    total = term if total is None else total + term
            out_ref[:, g * cols + w * 128:g * cols + (w + 1) * 128] = total.astype(BF)
    for copy in waits:
        copy.wait_send()


def kernel_form(tokens, expert_ids, slots, mix_weights, w_gate, w_up, w_down):
    experts, groups = lax.axis_size("expert"), lax.axis_size("dp")
    planes = groups // PLANE
    units = experts * planes
    rows = units * CAP
    tok_rows, width = tokens.shape
    hid = w_gate.shape[2]
    cols = w_down.shape[2]
    half = width // HALVES
    chunk_count = rows // CAP
    chunk = half // chunk_count
    everyone = experts * groups
    dma = pltpu.SemaphoreType.DMA
    return pl.pallas_call(
        functools.partial(kernel, experts, groups),
        out_shape=jax.ShapeDtypeStruct((tok_rows, width), BF),
        in_specs=[pl.BlockSpec(memory_space=pltpu.VMEM)] * 4
        + [pl.BlockSpec(memory_space=pl.ANY)] * 3,
        out_specs=pl.BlockSpec(memory_space=pltpu.VMEM),
        scratch_shapes=[
            pltpu.VMEM((width, hid), BF),
            pltpu.VMEM((width, hid), BF),
            pltpu.VMEM((groups, hid, cols), BF),
            pltpu.VMEM((HALVES, experts, rows, chunk), BF),
            pltpu.VMEM((HALVES, units, rows, chunk), BF),
            pltpu.VMEM((HALVES, PLANE, rows, half), BF),
            pltpu.VMEM((groups, PLANE * rows, hid), BF),
            pltpu.VMEM((everyone, cols // 128 * CAP, 128), BF),
            pltpu.VMEM((everyone, cols // 128 * CAP, 128), BF),
            dma((2 * HALVES + groups,)),
            dma((HALVES, units)), dma((HALVES, units)),
            dma((HALVES,)), dma((HALVES,)),
            dma((HALVES, 2)), dma((HALVES, 2)),
            dma((planes,)), dma((planes,)),
            dma((planes,)), dma((planes,)),
            dma((2 * planes,)), dma((planes, 2)),
            dma((everyone,)), dma((everyone,)),
        ],
        compiler_params=pltpu.CompilerParams(
            collective_id=0, has_side_effects=True, vmem_limit_bytes=56 * 2 ** 20
        ),
    )(tokens, expert_ids, slots, mix_weights, w_gate, w_up, w_down)


def solution(mesh):
    experts, groups = mesh.shape["expert"], mesh.shape["dp"]

    def shards(tokens, expert_ids, slots, mix_weights, w_gate, w_up, w_down):
        rows = experts * (groups // PLANE) * CAP
        fits = (
            groups % PLANE == 0
            and rows == 16
            and tokens.shape[0] % 8 == 0
            and tokens.shape[1] % (HALVES * (rows // CAP) * 128) == 0
            and w_gate.shape[2] % 128 == 0
            and w_down.shape[2] % 128 == 0
        )
        form = kernel_form if fits else collective_form
        return form(tokens, expert_ids, slots, mix_weights, w_gate, w_up, w_down)

    placed = (
        P(("expert", "dp"), None),
        P(("expert", "dp"), None),
        P(("expert", "dp"), None),
        P(("expert", "dp"), None),
        P("expert", None, "dp"),
        P("expert", None, "dp"),
        P("expert", None, "dp"),
    )
    return jax.shard_map(
        shards, mesh=mesh, in_specs=placed, out_specs=P(("expert", "dp"), None), check_vma=False
    )
```

```python
import functools

import jax
import jax.numpy as jnp
from jax import lax
from jax.experimental import pallas as pl
from jax.experimental.pallas import tpu as pltpu
from jax.sharding import PartitionSpec as P

CAP = 2
PLANE = 4
HALVES = 2
BF = jnp.bfloat16
F32 = jnp.float32


def collective_form(tokens, expert_ids, slots, mix_weights, w_gate, w_up, w_down):
    tok_rows, model_width = tokens.shape
    experts = lax.axis_size("expert")
    slot_count = experts * CAP
    slot_ids = jnp.arange(slot_count, dtype=jnp.int32)
    matches = (expert_ids[None, :, :] == (slot_ids // CAP)[:, None, None]) & (
        slots[None, :, :] == (slot_ids % CAP)[:, None, None]
    )
    table = jnp.any(matches, axis=2).astype(BF)
    outgoing = jnp.dot(table, tokens, preferred_element_type=F32).astype(BF)
    arrived = lax.all_to_all(outgoing, "expert", split_axis=0, concat_axis=0, tiled=True)
    portion = lax.all_gather(arrived, "dp", axis=0, tiled=True)
    gate_part = jnp.dot(portion, w_gate[0], preferred_element_type=F32)
    up_part = jnp.dot(portion, w_up[0], preferred_element_type=F32)
    hidden = (jax.nn.silu(gate_part) * up_part).astype(BF)
    summed = jnp.dot(
        lax.all_gather(hidden, "dp", axis=1, tiled=True), w_down[0], preferred_element_type=F32
    )
    result = summed.astype(BF)
    blocks = result.reshape(lax.axis_size("dp"), experts, CAP, result.shape[1])
    blocks = lax.all_to_all(blocks, "expert", split_axis=1, concat_axis=1, tiled=True)
    blocks = lax.all_to_all(blocks, "dp", split_axis=0, concat_axis=3, tiled=True)
    returned = blocks.reshape(slot_count, model_width)
    weight_table = jnp.sum(jnp.where(matches, mix_weights[None, :, :], 0.0), axis=2)
    mixed = jnp.dot(
        weight_table.T,
        returned.astype(F32),
        precision=lax.Precision.HIGHEST,
        preferred_element_type=F32,
    )
    return mixed.astype(BF)


def kernel(
    experts, groups,
    tok_ref, ids_ref, slot_ref, mix_ref, wg_hbm, wu_hbm, wd_hbm, out_ref,
    wg, wu, wd, obuf, ubuf, xbuf, hbuf, pbuf, rbuf,
    wsem, s1s, s1r, s2s, s2r, s3s, s3r, azs, azr, ays, ayr, acs, acr, rs, rr,
):
    planes = groups // PLANE
    units = experts * planes
    rows = units * CAP
    tok_rows, width = tok_ref.shape
    half = width // HALVES
    chunk_count = rows // CAP
    chunk = half // chunk_count
    cols = wd.shape[2]
    x = lax.axis_index("expert")
    d = lax.axis_index("dp")
    z, b = d // PLANE, d % PLANE
    y, c = b // 2, b % 2
    unit = x * planes + z
    y_block = (1 - y) * 2 + c
    c_block = y * 2 + 1 - c
    yc_block = (1 - y) * 2 + 1 - c

    def dev(xx, dd):
        return (xx, dd)

    def rdma(src, dst, ssem, rsem, device):
        return pltpu.make_async_remote_copy(
            src_ref=src, dst_ref=dst, send_sem=ssem, recv_sem=rsem,
            device_id=device, device_id_type=pl.DeviceIdType.MESH,
        )

    y_dev = dev(x, z * PLANE + y_block)
    c_dev = dev(x, z * PLANE + c_block)
    offsets = [(dx, dz) for dz in range(planes) for dx in range(experts) if dx or dz]

    def peer(dx, dz):
        return lax.rem(x + dx, experts), lax.rem(z + dz, planes)

    barrier = pltpu.get_barrier_semaphore()
    for dx, dz in offsets:
        px, pz = peer(dx, dz)
        pl.semaphore_signal(barrier, inc=1, device_id=dev(px, pz * PLANE + b),
                            device_id_type=pl.DeviceIdType.MESH)
    for other in (y_dev, c_dev):
        pl.semaphore_signal(barrier, inc=1, device_id=other,
                            device_id_type=pl.DeviceIdType.MESH)

    loads = []
    for h in range(HALVES):
        part = pl.ds(h * half, half)
        loads.append(pltpu.make_async_copy(wg_hbm.at[0, part], wg.at[part], wsem.at[2 * h]))
        loads.append(pltpu.make_async_copy(wu_hbm.at[0, part], wu.at[part], wsem.at[2 * h + 1]))
    depth = wd.shape[1]
    for g in range(groups):
        loads.append(pltpu.make_async_copy(
            wd_hbm.at[0, pl.ds(g * depth, depth)], wd.at[g], wsem.at[2 * HALVES + g]))
    for load in loads:
        load.start()

    lanes = experts * chunk_count * CAP
    ids = jnp.concatenate([ids_ref[...]] * (128 // tok_rows), axis=1)
    places = jnp.concatenate([slot_ref[...]] * (128 // tok_rows), axis=1)
    mix = jnp.concatenate([mix_ref[...]] * (128 // tok_rows), axis=1)
    row = lax.broadcasted_iota(jnp.int32, (lanes, 128), 0)
    row_e, row_j, row_r = row // rows, (row // CAP) % chunk_count, row % CAP
    column_j = lax.broadcasted_iota(jnp.int32, (lanes, 128), 1) // tok_rows
    pick = jnp.zeros((lanes, 128), F32)
    table = jnp.zeros((8, 128), F32)
    wide_row = lax.broadcasted_iota(jnp.int32, (8, 128), 0)
    for k in range(ids_ref.shape[0]):
        ids_k, places_k, mix_k = ids[k:k + 1], places[k:k + 1], mix[k:k + 1]
        pick = jnp.where((ids_k == row_e) & (places_k == row_r) & (column_j == row_j), 1.0, pick)
        table += jnp.where((ids_k == wide_row // CAP) & (places_k == wide_row % CAP), mix_k, 0.0)
    pick = pick[:, :chunk_count * tok_rows].astype(BF)
    table = table.T
    for h in range(HALVES):
        stack = jnp.concatenate(
            [tok_ref[:, h * half + j * chunk: h * half + (j + 1) * chunk].astype(F32)
             for j in range(chunk_count)], axis=0).astype(BF)
        sent = jnp.dot(pick, stack, preferred_element_type=F32).astype(BF)
        for e in range(experts):
            obuf[h, e] = sent[e * rows:(e + 1) * rows]
    weight_cols = {(e, r): table[:tok_rows, e * CAP + r:e * CAP + r + 1]
                   for e in range(experts) for r in range(CAP)}

    pl.semaphore_wait(barrier, len(offsets) + 2)

    waits = []
    for h in range(HALVES):
        for n, (dx, dz) in reversed(list(enumerate(offsets))):
            px, pz = peer(dx, dz)
            copy = rdma(obuf.at[h, px], ubuf.at[h, unit], s1s.at[h, n], s1r.at[h, unit],
                        dev(px, pz * PLANE + b))
            copy.start()
            waits.append(copy)
    for h in range(HALVES):
        ubuf[h, unit] = obuf[h, x]

    count = units * chunk_count * CAP
    pr = lax.broadcasted_iota(jnp.int32, (count, count), 0)
    pc = lax.broadcasted_iota(jnp.int32, (count, count), 1)
    source = ((pr // CAP) % units) * (chunk_count * CAP) + (pr // rows) * CAP + pr % CAP
    order = jnp.where(pc == source, 1.0, 0.0).astype(BF)

    def arrival(buf, h, slot, rsem):
        return rdma(buf, buf, s2s.at[0], rsem, y_dev)

    gate = up = None
    for h in range(HALVES):
        for dx, dz in offsets:
            px, pz = peer(dx, dz)
            pu = px * planes + pz
            rdma(ubuf.at[h, pu], ubuf.at[h, pu], s1s.at[0, 0], s1r.at[h, pu], y_dev).wait_recv()
        arrived = ubuf[h].reshape(count, chunk)
        block = jnp.dot(order, arrived, preferred_element_type=F32).astype(BF)
        for j in range(chunk_count):
            xbuf[h, b, :, j * chunk:(j + 1) * chunk] = block[j * rows:(j + 1) * rows]
        mine = xbuf.at[h, b]
        to_y = rdma(mine, mine, s2s.at[h], s2r.at[h], y_dev)
        to_y.start()
        to_c = rdma(mine, mine, s3s.at[h, 0], s3r.at[h, 0], c_dev)
        to_c.start()
        waits += [to_y, to_c]
    for h in range(HALVES):
        theirs = xbuf.at[h, y_block]
        rdma(theirs, theirs, s2s.at[h], s2r.at[h], y_dev).wait_recv()
        forward = rdma(theirs, theirs, s3s.at[h, 1], s3r.at[h, 1], c_dev)
        forward.start()
        waits.append(forward)
        for n, blk in enumerate((c_block, yc_block)):
            got = xbuf.at[h, blk]
            rdma(got, got, s3s.at[h, n], s3r.at[h, n], c_dev).wait_recv()
        loads[2 * h].wait()
        loads[2 * h + 1].wait()
        part = pl.ds(h * half, half)
        slab = xbuf[h].reshape(PLANE * rows, half)
        g_part = jnp.dot(slab, wg[part], preferred_element_type=F32)
        u_part = jnp.dot(slab, wu[part], preferred_element_type=F32)
        gate = g_part if gate is None else gate + g_part
        up = u_part if up is None else up + u_part
    hidden = (gate / (1.0 + jnp.exp(-gate)) * up).astype(BF)
    hbuf[d] = hidden

    def dp_of(zz, blk):
        return zz * PLANE + blk

    shard = hbuf.at[d]
    for dz in range(planes - 1, 0, -1):
        pz = lax.rem(z + dz, planes)
        copy = rdma(shard, shard, azs.at[dz], azr.at[z], dev(x, dp_of(pz, b)))
        copy.start()
        waits.append(copy)
    copy = rdma(shard, shard, ays.at[0], ayr.at[z], y_dev)
    copy.start()
    waits.append(copy)
    copy = rdma(shard, shard, acs.at[0], acr.at[z, 0], c_dev)
    copy.start()
    waits.append(copy)
    for load in loads[2 * HALVES:]:
        load.wait()

    def product(g):
        return jnp.dot(hbuf[g], wd[g], preferred_element_type=F32)

    acc = product(d)
    for dz in range(planes):
        pz = lax.rem(z + dz, planes)
        if dz:
            g = dp_of(pz, b)
            got = hbuf.at[g]
            rdma(got, got, azs.at[dz], azr.at[pz], y_dev).wait_recv()
            on_y = rdma(got, got, ays.at[dz], ayr.at[pz], y_dev)
            on_y.start()
            on_c = rdma(got, got, acs.at[dz], acr.at[pz, 0], c_dev)
            on_c.start()
            waits += [on_y, on_c]
            acc += product(g)
        g = dp_of(pz, c_block)
        got = hbuf.at[g]
        rdma(got, got, acs.at[0], acr.at[pz, 0], c_dev).wait_recv()
        acc += product(g)
    for dz in range(planes):
        pz = lax.rem(z + dz, planes)
        g = dp_of(pz, y_block)
        got = hbuf.at[g]
        rdma(got, got, ays.at[0], ayr.at[pz], y_dev).wait_recv()
        on_c = rdma(got, got, acs.at[planes + dz], acr.at[pz, 1], c_dev)
        on_c.start()
        waits.append(on_c)
        acc += product(g)
    for dz in range(planes):
        pz = lax.rem(z + dz, planes)
        g = dp_of(pz, yc_block)
        got = hbuf.at[g]
        rdma(got, got, acs.at[0], acr.at[pz, 1], c_dev).wait_recv()
        acc += product(g)

    wide = cols // 128
    piece_rows = wide * CAP
    everyone = experts * groups
    result = acc.astype(BF)
    for w in range(wide):
        for p in range(everyone):
            pbuf[p, w * CAP:(w + 1) * CAP, :] = result[p * CAP:(p + 1) * CAP,
                                                       w * 128:(w + 1) * 128]
    me = x * groups + d

    def piece_of(device):
        dx, dd = device // groups, device % groups
        return (dd % PLANE) * units + dx * planes + dd // PLANE

    rbuf[me] = pbuf[piece_of(me)]
    for k in range(1, everyone):
        other = lax.rem(me + k, everyone)
        copy = rdma(pbuf.at[piece_of(other)], rbuf.at[me], rs.at[k], rr.at[me],
                    dev(other // groups, other % groups))
        copy.start()
        waits.append(copy)
    for k in range(1, everyone):
        other = lax.rem(me + k, everyone)
        rdma(rbuf.at[other], rbuf.at[other], rs.at[k], rr.at[other], y_dev).wait_recv()
    for g in range(groups):
        pieces = [rbuf[e * groups + g].astype(F32) for e in range(experts)]
        for w in range(wide):
            total = None
            for e in range(experts):
                for r in range(CAP):
                    term = weight_cols[e, r] * pieces[e][w * CAP + r:w * CAP + r + 1]
                    total = term if total is None else total + term
            out_ref[:, g * cols + w * 128:g * cols + (w + 1) * 128] = total.astype(BF)
    for copy in waits:
        copy.wait_send()


def kernel_form(tokens, expert_ids, slots, mix_weights, w_gate, w_up, w_down):
    experts, groups = lax.axis_size("expert"), lax.axis_size("dp")
    planes = groups // PLANE
    units = experts * planes
    rows = units * CAP
    tok_rows, width = tokens.shape
    hid = w_gate.shape[2]
    cols = w_down.shape[2]
    half = width // HALVES
    chunk_count = rows // CAP
    chunk = half // chunk_count
    everyone = experts * groups
    dma = pltpu.SemaphoreType.DMA
    return pl.pallas_call(
        functools.partial(kernel, experts, groups),
        out_shape=jax.ShapeDtypeStruct((tok_rows, width), BF),
        in_specs=[pl.BlockSpec(memory_space=pltpu.VMEM)] * 4
        + [pl.BlockSpec(memory_space=pl.ANY)] * 3,
        out_specs=pl.BlockSpec(memory_space=pltpu.VMEM),
        scratch_shapes=[
            pltpu.VMEM((width, hid), BF),
            pltpu.VMEM((width, hid), BF),
            pltpu.VMEM((groups, hid, cols), BF),
            pltpu.VMEM((HALVES, experts, rows, chunk), BF),
            pltpu.VMEM((HALVES, units, rows, chunk), BF),
            pltpu.VMEM((HALVES, PLANE, rows, half), BF),
            pltpu.VMEM((groups, PLANE * rows, hid), BF),
            pltpu.VMEM((everyone, cols // 128 * CAP, 128), BF),
            pltpu.VMEM((everyone, cols // 128 * CAP, 128), BF),
            dma((2 * HALVES + groups,)),
            dma((HALVES, units)), dma((HALVES, units)),
            dma((HALVES,)), dma((HALVES,)),
            dma((HALVES, 2)), dma((HALVES, 2)),
            dma((planes,)), dma((planes,)),
            dma((planes,)), dma((planes,)),
            dma((2 * planes,)), dma((planes, 2)),
            dma((everyone,)), dma((everyone,)),
        ],
        compiler_params=pltpu.CompilerParams(
            collective_id=0, has_side_effects=True, vmem_limit_bytes=56 * 2 ** 20
        ),
    )(tokens, expert_ids.T, slots.T, mix_weights.T, w_gate, w_up, w_down)


def solution(mesh):
    experts, groups = mesh.shape["expert"], mesh.shape["dp"]

    def shards(tokens, expert_ids, slots, mix_weights, w_gate, w_up, w_down):
        rows = experts * (groups // PLANE) * CAP
        fits = (
            groups % PLANE == 0
            and rows == 16
            and tokens.shape[0] == 8
            and experts * CAP <= 8
            and tokens.shape[1] % (HALVES * (rows // CAP) * 128) == 0
            and w_gate.shape[2] % 128 == 0
            and w_down.shape[2] % 128 == 0
        )
        form = kernel_form if fits else collective_form
        return form(tokens, expert_ids, slots, mix_weights, w_gate, w_up, w_down)

    placed = (
        P(("expert", "dp"), None),
        P(("expert", "dp"), None),
        P(("expert", "dp"), None),
        P(("expert", "dp"), None),
        P("expert", None, "dp"),
        P("expert", None, "dp"),
        P("expert", None, "dp"),
    )
    return jax.shard_map(
        shards, mesh=mesh, in_specs=placed, out_specs=P(("expert", "dp"), None), check_vma=False
    )
```

```python
import functools

import jax
import jax.numpy as jnp
from jax import lax
from jax.experimental import pallas as pl
from jax.experimental.pallas import tpu as pltpu
from jax.sharding import PartitionSpec as P

CAP = 2
PLANE = 4
PARTS = 1
HALVES = 2
BF = jnp.bfloat16
F32 = jnp.float32


def collective_form(tokens, expert_ids, slots, mix_weights, w_gate, w_up, w_down):
    tok_rows, model_width = tokens.shape
    experts = lax.axis_size("expert")
    slot_count = experts * CAP
    slot_ids = jnp.arange(slot_count, dtype=jnp.int32)
    matches = (expert_ids[None, :, :] == (slot_ids // CAP)[:, None, None]) & (
        slots[None, :, :] == (slot_ids % CAP)[:, None, None]
    )
    table = jnp.any(matches, axis=2).astype(BF)
    outgoing = jnp.dot(table, tokens, preferred_element_type=F32).astype(BF)
    arrived = lax.all_to_all(outgoing, "expert", split_axis=0, concat_axis=0, tiled=True)
    portion = lax.all_gather(arrived, "dp", axis=0, tiled=True)
    gate_part = jnp.dot(portion, w_gate[0], preferred_element_type=F32)
    up_part = jnp.dot(portion, w_up[0], preferred_element_type=F32)
    hidden = (jax.nn.silu(gate_part) * up_part).astype(BF)
    summed = jnp.dot(
        lax.all_gather(hidden, "dp", axis=1, tiled=True), w_down[0], preferred_element_type=F32
    )
    result = summed.astype(BF)
    blocks = result.reshape(lax.axis_size("dp"), experts, CAP, result.shape[1])
    blocks = lax.all_to_all(blocks, "expert", split_axis=1, concat_axis=1, tiled=True)
    blocks = lax.all_to_all(blocks, "dp", split_axis=0, concat_axis=3, tiled=True)
    returned = blocks.reshape(slot_count, model_width)
    weight_table = jnp.sum(jnp.where(matches, mix_weights[None, :, :], 0.0), axis=2)
    mixed = jnp.dot(
        weight_table.T,
        returned.astype(F32),
        precision=lax.Precision.HIGHEST,
        preferred_element_type=F32,
    )
    return mixed.astype(BF)


def kernel(
    experts, groups,
    tok_hbm, ids_hbm, slot_hbm, mix_hbm, wg_hbm, wu_hbm, wd_hbm, out_ref,
    tok_ref, ids_ref, slot_ref, mix_ref, tsem, wg, wu, wd, obuf, ubuf, xbuf, hbuf, pbuf, rbuf,
    wsem, s1s, s1r, s2s, s2r, s3s, s3r, azs, azr, ays, ayr, acs, acr, rs, rr,
):
    planes = groups // PLANE
    units = experts * planes
    rows = units * CAP
    tok_rows, width = tok_ref.shape
    half = width // HALVES
    chunk_count = rows // CAP
    chunk = half // chunk_count
    cols = wd.shape[2]
    x = lax.axis_index("expert")
    d = lax.axis_index("dp")
    z, b = d // PLANE, d % PLANE
    y, c = b // 2, b % 2
    unit = x * planes + z
    y_block = (1 - y) * 2 + c
    c_block = y * 2 + 1 - c
    yc_block = (1 - y) * 2 + 1 - c

    def dev(xx, dd):
        return (xx, dd)

    def rdma(src, dst, ssem, rsem, device):
        return pltpu.make_async_remote_copy(
            src_ref=src, dst_ref=dst, send_sem=ssem, recv_sem=rsem,
            device_id=device, device_id_type=pl.DeviceIdType.MESH,
        )

    y_dev = dev(x, z * PLANE + y_block)
    c_dev = dev(x, z * PLANE + c_block)
    offsets = [(dx, dz) for dz in range(planes) for dx in range(experts) if dx or dz]
    step = 1 - 2 * (z // 2)
    far = (planes - 1) * (1 - z // 2)
    middle = ((z + 1) // 2) % 2
    targets = [far, far - step, far - 2 * step - middle * step]

    def peer(dx, dz):
        return lax.rem(x + dx, experts), lax.rem(z + dz, planes)

    barrier = pltpu.get_barrier_semaphore()
    for dx, dz in offsets:
        px, pz = peer(dx, dz)
        pl.semaphore_signal(barrier, inc=1, device_id=dev(px, pz * PLANE + b),
                            device_id_type=pl.DeviceIdType.MESH)
    for other in (y_dev, c_dev):
        pl.semaphore_signal(barrier, inc=1, device_id=other,
                            device_id_type=pl.DeviceIdType.MESH)

    small = [pltpu.make_async_copy(src, dst, tsem.at[n]) for n, (src, dst) in enumerate(
        ((ids_hbm, ids_ref), (slot_hbm, slot_ref), (mix_hbm, mix_ref), (tok_hbm, tok_ref)))]
    for load in small:
        load.start()
    loads = []
    for h in range(HALVES):
        part = pl.ds(h * half, half)
        loads.append(pltpu.make_async_copy(wg_hbm.at[0, part], wg.at[part], wsem.at[2 * h]))
        loads.append(pltpu.make_async_copy(wu_hbm.at[0, part], wu.at[part], wsem.at[2 * h + 1]))
    depth = wd.shape[1]
    for g in range(groups):
        loads.append(pltpu.make_async_copy(
            wd_hbm.at[0, pl.ds(g * depth, depth)], wd.at[g], wsem.at[2 * HALVES + g]))

    for load in small[:3]:
        load.wait()
    lanes = experts * chunk_count * CAP
    ids = jnp.concatenate([ids_ref[...]] * (128 // tok_rows), axis=1)
    places = jnp.concatenate([slot_ref[...]] * (128 // tok_rows), axis=1)
    mix = jnp.concatenate([mix_ref[...]] * (128 // tok_rows), axis=1)
    row = lax.broadcasted_iota(jnp.int32, (lanes, 128), 0)
    row_e, row_j, row_r = row // rows, (row // CAP) % chunk_count, row % CAP
    column_j = lax.broadcasted_iota(jnp.int32, (lanes, 128), 1) // tok_rows
    pick = jnp.zeros((lanes, 128), F32)
    table = jnp.zeros((8, 128), F32)
    wide_row = lax.broadcasted_iota(jnp.int32, (8, 128), 0)
    for k in range(ids_ref.shape[0]):
        ids_k, places_k, mix_k = ids[k:k + 1], places[k:k + 1], mix[k:k + 1]
        pick = jnp.where((ids_k == row_e) & (places_k == row_r) & (column_j == row_j), 1.0, pick)
        table += jnp.where((ids_k == wide_row // CAP) & (places_k == wide_row % CAP), mix_k, 0.0)
    pick = pick[:, :chunk_count * tok_rows].astype(BF)
    table = table.T
    small[3].wait()
    for h in range(HALVES):
        stack = jnp.concatenate(
            [tok_ref[:, h * half + j * chunk: h * half + (j + 1) * chunk].astype(F32)
             for j in range(chunk_count)], axis=0).astype(BF)
        sent = jnp.dot(pick, stack, preferred_element_type=F32).astype(BF)
        for e in range(experts):
            obuf[h, e] = sent[e * rows:(e + 1) * rows]
    weight_cols = {(e, r): table[:tok_rows, e * CAP + r:e * CAP + r + 1]
                   for e in range(experts) for r in range(CAP)}

    for load in loads:
        load.start()
    pl.semaphore_wait(barrier, len(offsets) + 2)

    waits = []
    for h in range(HALVES):
        stops = [(lax.rem(x + dx, experts), pz) for pz in targets
                 for dx in range(experts - 1, -1, -1)]
        stops += [peer(dx, 0) for dx in range(1, experts)]
        for n, (px, pz) in enumerate(stops):
            copy = rdma(obuf.at[h, px], ubuf.at[h, unit], s1s.at[h, n], s1r.at[h, unit],
                        dev(px, pz * PLANE + b))
            copy.start()
            waits.append(copy)
    for h in range(HALVES):
        ubuf[h, unit] = obuf[h, x]

    count = units * chunk_count * CAP
    pr = lax.broadcasted_iota(jnp.int32, (count, count), 0)
    pc = lax.broadcasted_iota(jnp.int32, (count, count), 1)
    source = ((pr // CAP) % units) * (chunk_count * CAP) + (pr // rows) * CAP + pr % CAP
    order = jnp.where(pc == source, 1.0, 0.0).astype(BF)

    def arrival(buf, h, slot, rsem):
        return rdma(buf, buf, s2s.at[0], rsem, y_dev)

    gate = up = None
    for h in range(HALVES):
        for dx, dz in offsets:
            px, pz = peer(dx, dz)
            pu = px * planes + pz
            rdma(ubuf.at[h, pu], ubuf.at[h, pu], s1s.at[0, 0], s1r.at[h, pu], y_dev).wait_recv()
        arrived = ubuf[h].reshape(count, chunk)
        block = jnp.dot(order, arrived, preferred_element_type=F32).astype(BF)
        for j in range(chunk_count):
            xbuf[h, b, :, j * chunk:(j + 1) * chunk] = block[j * rows:(j + 1) * rows]
        mine = xbuf.at[h, b]
        to_y = rdma(mine, mine, s2s.at[h], s2r.at[h], y_dev)
        to_y.start()
        to_c = rdma(mine, mine, s3s.at[h, 0], s3r.at[h, 0], c_dev)
        to_c.start()
        waits += [to_y, to_c]
    for h in range(HALVES):
        theirs = xbuf.at[h, y_block]
        rdma(theirs, theirs, s2s.at[h], s2r.at[h], y_dev).wait_recv()
        forward = rdma(theirs, theirs, s3s.at[h, 1], s3r.at[h, 1], c_dev)
        forward.start()
        waits.append(forward)
        for n, blk in enumerate((c_block, yc_block)):
            got = xbuf.at[h, blk]
            rdma(got, got, s3s.at[h, n], s3r.at[h, n], c_dev).wait_recv()
        loads[2 * h].wait()
        loads[2 * h + 1].wait()
        part = pl.ds(h * half, half)
        slab = xbuf[h].reshape(PLANE * rows, half)
        g_part = jnp.dot(slab, wg[part], preferred_element_type=F32)
        u_part = jnp.dot(slab, wu[part], preferred_element_type=F32)
        gate = g_part if gate is None else gate + g_part
        up = u_part if up is None else up + u_part
    hidden = (gate / (1.0 + jnp.exp(-gate)) * up).astype(BF)
    piece = hbuf.shape[3]
    for i in range(PARTS):
        hbuf[d, i] = hidden[:, i * piece:(i + 1) * piece]

    def dp_of(zz, blk):
        return zz * PLANE + blk

    def send(g, i, ssem, rsem, device):
        ref = hbuf.at[g, i]
        copy = rdma(ref, ref, ssem, rsem, device)
        copy.start()
        waits.append(copy)

    def receive(g, i, rsem):
        ref = hbuf.at[g, i]
        rdma(ref, ref, acs.at[0, 0], rsem, y_dev).wait_recv()

    for i in range(PARTS):
        send(d, i, ays.at[0, i], ayr.at[z, i], y_dev)
        for n, pz in enumerate(targets):
            send(d, i, azs.at[n, i], azr.at[z, i], dev(x, dp_of(pz, b)))
        send(d, i, acs.at[0, i], acr.at[z, 0, i], c_dev)
    for load in loads[2 * HALVES:]:
        load.wait()

    def product(g, i):
        return jnp.dot(hbuf[g, i], wd[g, i * piece:(i + 1) * piece],
                       preferred_element_type=F32)

    acc = None
    for i in range(PARTS):
        acc = product(d, i) if acc is None else acc + product(d, i)
    near = [z] + targets[::-1]

    def drain(i):
        total = None
        for n, pz in enumerate(near):
            if n:
                g = dp_of(pz, y_block)
                receive(g, i, ayr.at[pz, i])
                send(g, i, acs.at[planes + n, i], acr.at[pz, 1, i], c_dev)
                term = product(g, i)
                total = term if total is None else total + term
        for n, pz in enumerate(near):
            g = dp_of(pz, yc_block)
            receive(g, i, acr.at[pz, 1, i])
            total += product(g, i)
        return total

    for i in range(PARTS):
        for n, pz in enumerate(near):
            g = dp_of(pz, b)
            if n:
                receive(g, i, azr.at[pz, i])
                send(g, i, ays.at[n, i], ayr.at[pz, i], y_dev)
                send(g, i, acs.at[n, i], acr.at[pz, 0, i], c_dev)
                acc += product(g, i)
            g = dp_of(pz, y_block)
            if not n:
                receive(g, i, ayr.at[pz, i])
                send(g, i, acs.at[planes + n, i], acr.at[pz, 1, i], c_dev)
                acc += product(g, i)
            g = dp_of(pz, c_block)
            receive(g, i, acr.at[pz, 0, i])
            acc += product(g, i)
        if i:
            acc += drain(i - 1)
    acc += drain(PARTS - 1)

    wide = cols // 128
    piece_rows = wide * CAP
    everyone = experts * groups
    result = acc.astype(BF)
    for w in range(wide):
        for p in range(everyone):
            pbuf[p, w * CAP:(w + 1) * CAP, :] = result[p * CAP:(p + 1) * CAP,
                                                       w * 128:(w + 1) * 128]
    me = x * groups + d

    def piece_of(device):
        dx, dd = device // groups, device % groups
        return (dd % PLANE) * units + dx * planes + dd // PLANE

    rbuf[me] = pbuf[piece_of(me)]
    for k in range(1, everyone):
        other = lax.rem(me + k, everyone)
        copy = rdma(pbuf.at[piece_of(other)], rbuf.at[me], rs.at[k], rr.at[me],
                    dev(other // groups, other % groups))
        copy.start()
        waits.append(copy)
    for k in range(1, everyone):
        other = lax.rem(me + k, everyone)
        rdma(rbuf.at[other], rbuf.at[other], rs.at[k], rr.at[other], y_dev).wait_recv()
    for g in range(groups):
        pieces = [rbuf[e * groups + g].astype(F32) for e in range(experts)]
        for w in range(wide):
            total = None
            for e in range(experts):
                for r in range(CAP):
                    term = weight_cols[e, r] * pieces[e][w * CAP + r:w * CAP + r + 1]
                    total = term if total is None else total + term
            out_ref[:, g * cols + w * 128:g * cols + (w + 1) * 128] = total.astype(BF)
    for copy in waits:
        copy.wait_send()


def kernel_form(tokens, expert_ids, slots, mix_weights, w_gate, w_up, w_down):
    experts, groups = lax.axis_size("expert"), lax.axis_size("dp")
    planes = groups // PLANE
    units = experts * planes
    rows = units * CAP
    tok_rows, width = tokens.shape
    hid = w_gate.shape[2]
    cols = w_down.shape[2]
    half = width // HALVES
    chunk_count = rows // CAP
    chunk = half // chunk_count
    everyone = experts * groups
    dma = pltpu.SemaphoreType.DMA
    return pl.pallas_call(
        functools.partial(kernel, experts, groups),
        out_shape=jax.ShapeDtypeStruct((tok_rows, width), BF),
        in_specs=[pl.BlockSpec(memory_space=pltpu.HBM)] * 7,
        out_specs=pl.BlockSpec(memory_space=pltpu.VMEM),
        scratch_shapes=[
            pltpu.VMEM((tok_rows, width), BF),
            pltpu.VMEM(expert_ids.shape[::-1], jnp.int32),
            pltpu.VMEM(slots.shape[::-1], jnp.int32),
            pltpu.VMEM(mix_weights.shape[::-1], F32),
            dma((4,)),
            pltpu.VMEM((width, hid), BF),
            pltpu.VMEM((width, hid), BF),
            pltpu.VMEM((groups, hid, cols), BF),
            pltpu.VMEM((HALVES, experts, rows, chunk), BF),
            pltpu.VMEM((HALVES, units, rows, chunk), BF),
            pltpu.VMEM((HALVES, PLANE, rows, half), BF),
            pltpu.VMEM((groups, PARTS, PLANE * rows, hid // PARTS), BF),
            pltpu.VMEM((everyone, cols // 128 * CAP, 128), BF),
            pltpu.VMEM((everyone, cols // 128 * CAP, 128), BF),
            dma((2 * HALVES + groups,)),
            dma((HALVES, units)), dma((HALVES, units)),
            dma((HALVES,)), dma((HALVES,)),
            dma((HALVES, 2)), dma((HALVES, 2)),
            dma((planes, PARTS)), dma((planes, PARTS)),
            dma((planes, PARTS)), dma((planes, PARTS)),
            dma((2 * planes, PARTS)), dma((planes, 2, PARTS)),
            dma((everyone,)), dma((everyone,)),
        ],
        compiler_params=pltpu.CompilerParams(
            collective_id=0, has_side_effects=True, vmem_limit_bytes=56 * 2 ** 20
        ),
    )(tokens, expert_ids.T, slots.T, mix_weights.T, w_gate, w_up, w_down)


def solution(mesh):
    experts, groups = mesh.shape["expert"], mesh.shape["dp"]

    def shards(tokens, expert_ids, slots, mix_weights, w_gate, w_up, w_down):
        rows = experts * (groups // PLANE) * CAP
        fits = (
            groups % PLANE == 0
            and rows == 16
            and groups == 4 * PLANE
            and tokens.shape[0] == 8
            and experts * CAP <= 8
            and tokens.shape[1] % (HALVES * (rows // CAP) * 128) == 0
            and w_gate.shape[2] % (128 * PARTS) == 0
            and w_down.shape[2] % 128 == 0
        )
        form = kernel_form if fits else collective_form
        return form(tokens, expert_ids, slots, mix_weights, w_gate, w_up, w_down)

    placed = (
        P(("expert", "dp"), None),
        P(("expert", "dp"), None),
        P(("expert", "dp"), None),
        P(("expert", "dp"), None),
        P("expert", None, "dp"),
        P("expert", None, "dp"),
        P("expert", None, "dp"),
    )
    return jax.shard_map(
        shards, mesh=mesh, in_specs=placed, out_specs=P(("expert", "dp"), None), check_vma=False
    )
```

```python
import functools

import jax
import jax.numpy as jnp
from jax import lax
from jax.experimental import pallas as pl
from jax.experimental.pallas import tpu as pltpu
from jax.sharding import PartitionSpec as P

CAP = 2
PLANE = 4
PARTS = 1
HALVES = 1
BF = jnp.bfloat16
F32 = jnp.float32


def collective_form(tokens, expert_ids, slots, mix_weights, w_gate, w_up, w_down):
    tok_rows, model_width = tokens.shape
    experts = lax.axis_size("expert")
    slot_count = experts * CAP
    slot_ids = jnp.arange(slot_count, dtype=jnp.int32)
    matches = (expert_ids[None, :, :] == (slot_ids // CAP)[:, None, None]) & (
        slots[None, :, :] == (slot_ids % CAP)[:, None, None]
    )
    table = jnp.any(matches, axis=2).astype(BF)
    outgoing = jnp.dot(table, tokens, preferred_element_type=F32).astype(BF)
    arrived = lax.all_to_all(outgoing, "expert", split_axis=0, concat_axis=0, tiled=True)
    portion = lax.all_gather(arrived, "dp", axis=0, tiled=True)
    gate_part = jnp.dot(portion, w_gate[0], preferred_element_type=F32)
    up_part = jnp.dot(portion, w_up[0], preferred_element_type=F32)
    hidden = (jax.nn.silu(gate_part) * up_part).astype(BF)
    summed = jnp.dot(
        lax.all_gather(hidden, "dp", axis=1, tiled=True), w_down[0], preferred_element_type=F32
    )
    result = summed.astype(BF)
    blocks = result.reshape(lax.axis_size("dp"), experts, CAP, result.shape[1])
    blocks = lax.all_to_all(blocks, "expert", split_axis=1, concat_axis=1, tiled=True)
    blocks = lax.all_to_all(blocks, "dp", split_axis=0, concat_axis=3, tiled=True)
    returned = blocks.reshape(slot_count, model_width)
    weight_table = jnp.sum(jnp.where(matches, mix_weights[None, :, :], 0.0), axis=2)
    mixed = jnp.dot(
        weight_table.T,
        returned.astype(F32),
        precision=lax.Precision.HIGHEST,
        preferred_element_type=F32,
    )
    return mixed.astype(BF)


def kernel(
    experts, groups,
    tok_hbm, ids_hbm, slot_hbm, mix_hbm, wg_hbm, wu_hbm, wd_hbm, out_ref,
    tok_ref, ids_ref, slot_ref, mix_ref, tsem, wg, wu, wd, obuf, ubuf, xbuf, hbuf, pbuf, rbuf,
    wsem, s1s, s1r, s2s, s2r, s3s, s3r, azs, azr, ays, ayr, acs, acr, rs, rr,
):
    planes = groups // PLANE
    units = experts * planes
    rows = units * CAP
    tok_rows, width = tok_ref.shape
    half = width // HALVES
    chunk_count = rows // CAP
    chunk = half // chunk_count
    cols = wd.shape[2]
    x = lax.axis_index("expert")
    d = lax.axis_index("dp")
    z, b = d // PLANE, d % PLANE
    y, c = b // 2, b % 2
    unit = x * planes + z
    y_block = (1 - y) * 2 + c
    c_block = y * 2 + 1 - c
    yc_block = (1 - y) * 2 + 1 - c

    def dev(xx, dd):
        return (xx, dd)

    def rdma(src, dst, ssem, rsem, device):
        return pltpu.make_async_remote_copy(
            src_ref=src, dst_ref=dst, send_sem=ssem, recv_sem=rsem,
            device_id=device, device_id_type=pl.DeviceIdType.MESH,
        )

    y_dev = dev(x, z * PLANE + y_block)
    c_dev = dev(x, z * PLANE + c_block)
    offsets = [(dx, dz) for dz in range(planes) for dx in range(experts) if dx or dz]
    step = 1 - 2 * (z // 2)
    far = (planes - 1) * (1 - z // 2)
    middle = ((z + 1) // 2) % 2
    targets = [far, far - step, far - 2 * step - middle * step]

    def peer(dx, dz):
        return lax.rem(x + dx, experts), lax.rem(z + dz, planes)

    barrier = pltpu.get_barrier_semaphore()
    for dx, dz in offsets:
        px, pz = peer(dx, dz)
        pl.semaphore_signal(barrier, inc=1, device_id=dev(px, pz * PLANE + b),
                            device_id_type=pl.DeviceIdType.MESH)
    for other in (y_dev, c_dev):
        pl.semaphore_signal(barrier, inc=1, device_id=other,
                            device_id_type=pl.DeviceIdType.MESH)

    small = [pltpu.make_async_copy(src, dst, tsem.at[n]) for n, (src, dst) in enumerate(
        ((ids_hbm, ids_ref), (slot_hbm, slot_ref), (mix_hbm, mix_ref), (tok_hbm, tok_ref)))]
    for load in small:
        load.start()
    loads = []
    for h in range(HALVES):
        part = pl.ds(h * half, half)
        loads.append(pltpu.make_async_copy(wg_hbm.at[0, part], wg.at[part], wsem.at[2 * h]))
        loads.append(pltpu.make_async_copy(wu_hbm.at[0, part], wu.at[part], wsem.at[2 * h + 1]))
    depth = wd.shape[1]
    for g in range(groups):
        loads.append(pltpu.make_async_copy(
            wd_hbm.at[0, pl.ds(g * depth, depth)], wd.at[g], wsem.at[2 * HALVES + g]))

    for load in small[:3]:
        load.wait()
    lanes = experts * chunk_count * CAP
    ids = jnp.concatenate([ids_ref[...]] * (128 // tok_rows), axis=1)
    places = jnp.concatenate([slot_ref[...]] * (128 // tok_rows), axis=1)
    mix = jnp.concatenate([mix_ref[...]] * (128 // tok_rows), axis=1)
    row = lax.broadcasted_iota(jnp.int32, (lanes, 128), 0)
    row_e, row_j, row_r = row // rows, (row // CAP) % chunk_count, row % CAP
    column_j = lax.broadcasted_iota(jnp.int32, (lanes, 128), 1) // tok_rows
    pick = jnp.zeros((lanes, 128), F32)
    table = jnp.zeros((8, 128), F32)
    wide_row = lax.broadcasted_iota(jnp.int32, (8, 128), 0)
    for k in range(ids_ref.shape[0]):
        ids_k, places_k, mix_k = ids[k:k + 1], places[k:k + 1], mix[k:k + 1]
        pick = jnp.where((ids_k == row_e) & (places_k == row_r) & (column_j == row_j), 1.0, pick)
        table += jnp.where((ids_k == wide_row // CAP) & (places_k == wide_row % CAP), mix_k, 0.0)
    pick = pick[:, :chunk_count * tok_rows].astype(BF)
    table = table.T
    small[3].wait()
    for h in range(HALVES):
        stack = jnp.concatenate(
            [tok_ref[:, h * half + j * chunk: h * half + (j + 1) * chunk].astype(F32)
             for j in range(chunk_count)], axis=0).astype(BF)
        sent = jnp.dot(pick, stack, preferred_element_type=F32).astype(BF)
        for e in range(experts):
            obuf[h, e] = sent[e * rows:(e + 1) * rows]
    weight_cols = {(e, r): table[:tok_rows, e * CAP + r:e * CAP + r + 1]
                   for e in range(experts) for r in range(CAP)}

    for load in loads:
        load.start()
    pl.semaphore_wait(barrier, len(offsets) + 2)

    waits = []
    for h in range(HALVES):
        stops = [(lax.rem(x + dx, experts), pz) for pz in targets
                 for dx in range(experts - 1, -1, -1)]
        stops += [peer(dx, 0) for dx in range(1, experts)]
        for n, (px, pz) in enumerate(stops):
            copy = rdma(obuf.at[h, px], ubuf.at[h, unit], s1s.at[h, n], s1r.at[h, unit],
                        dev(px, pz * PLANE + b))
            copy.start()
            waits.append(copy)
    for h in range(HALVES):
        ubuf[h, unit] = obuf[h, x]

    count = units * chunk_count * CAP
    pr = lax.broadcasted_iota(jnp.int32, (count, count), 0)
    pc = lax.broadcasted_iota(jnp.int32, (count, count), 1)
    source = ((pr // CAP) % units) * (chunk_count * CAP) + (pr // rows) * CAP + pr % CAP
    order = jnp.where(pc == source, 1.0, 0.0).astype(BF)

    def arrival(buf, h, slot, rsem):
        return rdma(buf, buf, s2s.at[0], rsem, y_dev)

    gate = up = None
    for h in range(HALVES):
        for dx, dz in offsets:
            px, pz = peer(dx, dz)
            pu = px * planes + pz
            rdma(ubuf.at[h, pu], ubuf.at[h, pu], s1s.at[0, 0], s1r.at[h, pu], y_dev).wait_recv()
        arrived = ubuf[h].reshape(count, chunk)
        block = jnp.dot(order, arrived, preferred_element_type=F32).astype(BF)
        for j in range(chunk_count):
            xbuf[h, b, :, j * chunk:(j + 1) * chunk] = block[j * rows:(j + 1) * rows]
        mine = xbuf.at[h, b]
        to_y = rdma(mine, mine, s2s.at[h], s2r.at[h], y_dev)
        to_y.start()
        to_c = rdma(mine, mine, s3s.at[h, 0], s3r.at[h, 0], c_dev)
        to_c.start()
        waits += [to_y, to_c]
    for h in range(HALVES):
        theirs = xbuf.at[h, y_block]
        rdma(theirs, theirs, s2s.at[h], s2r.at[h], y_dev).wait_recv()
        forward = rdma(theirs, theirs, s3s.at[h, 1], s3r.at[h, 1], c_dev)
        forward.start()
        waits.append(forward)
        for n, blk in enumerate((c_block, yc_block)):
            got = xbuf.at[h, blk]
            rdma(got, got, s3s.at[h, n], s3r.at[h, n], c_dev).wait_recv()
        loads[2 * h].wait()
        loads[2 * h + 1].wait()
        part = pl.ds(h * half, half)
        slab = xbuf[h].reshape(PLANE * rows, half)
        g_part = jnp.dot(slab, wg[part], preferred_element_type=F32)
        u_part = jnp.dot(slab, wu[part], preferred_element_type=F32)
        gate = g_part if gate is None else gate + g_part
        up = u_part if up is None else up + u_part
    hidden = (gate / (1.0 + jnp.exp(-gate)) * up).astype(BF)
    piece = hbuf.shape[3]
    for i in range(PARTS):
        hbuf[d, i] = hidden[:, i * piece:(i + 1) * piece]

    def dp_of(zz, blk):
        return zz * PLANE + blk

    def send(g, i, ssem, rsem, device):
        ref = hbuf.at[g, i]
        copy = rdma(ref, ref, ssem, rsem, device)
        copy.start()
        waits.append(copy)

    def receive(g, i, rsem):
        ref = hbuf.at[g, i]
        rdma(ref, ref, acs.at[0, 0], rsem, y_dev).wait_recv()

    for i in range(PARTS):
        send(d, i, ays.at[0, i], ayr.at[z, i], y_dev)
        for n, pz in enumerate(targets):
            send(d, i, azs.at[n, i], azr.at[z, i], dev(x, dp_of(pz, b)))
        send(d, i, acs.at[0, i], acr.at[z, 0, i], c_dev)
    for load in loads[2 * HALVES:]:
        load.wait()

    def product(g, i):
        return jnp.dot(hbuf[g, i], wd[g, i * piece:(i + 1) * piece],
                       preferred_element_type=F32)

    acc = None
    for i in range(PARTS):
        acc = product(d, i) if acc is None else acc + product(d, i)
    near = [z] + targets[::-1]

    def drain(i):
        total = None
        for n, pz in enumerate(near):
            if n:
                g = dp_of(pz, y_block)
                receive(g, i, ayr.at[pz, i])
                send(g, i, acs.at[planes + n, i], acr.at[pz, 1, i], c_dev)
                term = product(g, i)
                total = term if total is None else total + term
        for n, pz in enumerate(near):
            g = dp_of(pz, yc_block)
            receive(g, i, acr.at[pz, 1, i])
            total += product(g, i)
        return total

    for i in range(PARTS):
        for n, pz in enumerate(near):
            g = dp_of(pz, b)
            if n:
                receive(g, i, azr.at[pz, i])
                send(g, i, ays.at[n, i], ayr.at[pz, i], y_dev)
                send(g, i, acs.at[n, i], acr.at[pz, 0, i], c_dev)
                acc += product(g, i)
            g = dp_of(pz, y_block)
            if not n:
                receive(g, i, ayr.at[pz, i])
                send(g, i, acs.at[planes + n, i], acr.at[pz, 1, i], c_dev)
                acc += product(g, i)
            g = dp_of(pz, c_block)
            receive(g, i, acr.at[pz, 0, i])
            acc += product(g, i)
        if i:
            acc += drain(i - 1)
    acc += drain(PARTS - 1)

    wide = cols // 128
    piece_rows = wide * CAP
    everyone = experts * groups
    result = acc.astype(BF)
    for w in range(wide):
        for p in range(everyone):
            pbuf[p, w * CAP:(w + 1) * CAP, :] = result[p * CAP:(p + 1) * CAP,
                                                       w * 128:(w + 1) * 128]
    me = x * groups + d

    def piece_of(device):
        dx, dd = device // groups, device % groups
        return (dd % PLANE) * units + dx * planes + dd // PLANE

    rbuf[me] = pbuf[piece_of(me)]
    for k in range(1, everyone):
        other = lax.rem(me + k, everyone)
        copy = rdma(pbuf.at[piece_of(other)], rbuf.at[me], rs.at[k], rr.at[me],
                    dev(other // groups, other % groups))
        copy.start()
        waits.append(copy)
    for k in range(1, everyone):
        other = lax.rem(me + k, everyone)
        rdma(rbuf.at[other], rbuf.at[other], rs.at[k], rr.at[other], y_dev).wait_recv()
    for g in range(groups):
        pieces = [rbuf[e * groups + g].astype(F32) for e in range(experts)]
        for w in range(wide):
            total = None
            for e in range(experts):
                for r in range(CAP):
                    term = weight_cols[e, r] * pieces[e][w * CAP + r:w * CAP + r + 1]
                    total = term if total is None else total + term
            out_ref[:, g * cols + w * 128:g * cols + (w + 1) * 128] = total.astype(BF)
    for copy in waits:
        copy.wait_send()


def kernel_form(tokens, expert_ids, slots, mix_weights, w_gate, w_up, w_down):
    experts, groups = lax.axis_size("expert"), lax.axis_size("dp")
    planes = groups // PLANE
    units = experts * planes
    rows = units * CAP
    tok_rows, width = tokens.shape
    hid = w_gate.shape[2]
    cols = w_down.shape[2]
    half = width // HALVES
    chunk_count = rows // CAP
    chunk = half // chunk_count
    everyone = experts * groups
    dma = pltpu.SemaphoreType.DMA
    return pl.pallas_call(
        functools.partial(kernel, experts, groups),
        out_shape=jax.ShapeDtypeStruct((tok_rows, width), BF),
        in_specs=[pl.BlockSpec(memory_space=pltpu.HBM)] * 7,
        out_specs=pl.BlockSpec(memory_space=pltpu.VMEM),
        scratch_shapes=[
            pltpu.VMEM((tok_rows, width), BF),
            pltpu.VMEM(expert_ids.shape[::-1], jnp.int32),
            pltpu.VMEM(slots.shape[::-1], jnp.int32),
            pltpu.VMEM(mix_weights.shape[::-1], F32),
            dma((4,)),
            pltpu.VMEM((width, hid), BF),
            pltpu.VMEM((width, hid), BF),
            pltpu.VMEM((groups, hid, cols), BF),
            pltpu.VMEM((HALVES, experts, rows, chunk), BF),
            pltpu.VMEM((HALVES, units, rows, chunk), BF),
            pltpu.VMEM((HALVES, PLANE, rows, half), BF),
            pltpu.VMEM((groups, PARTS, PLANE * rows, hid // PARTS), BF),
            pltpu.VMEM((everyone, cols // 128 * CAP, 128), BF),
            pltpu.VMEM((everyone, cols // 128 * CAP, 128), BF),
            dma((2 * HALVES + groups,)),
            dma((HALVES, units)), dma((HALVES, units)),
            dma((HALVES,)), dma((HALVES,)),
            dma((HALVES, 2)), dma((HALVES, 2)),
            dma((planes, PARTS)), dma((planes, PARTS)),
            dma((planes, PARTS)), dma((planes, PARTS)),
            dma((2 * planes, PARTS)), dma((planes, 2, PARTS)),
            dma((everyone,)), dma((everyone,)),
        ],
        compiler_params=pltpu.CompilerParams(
            collective_id=0, has_side_effects=True, vmem_limit_bytes=56 * 2 ** 20
        ),
    )(tokens, expert_ids.T, slots.T, mix_weights.T, w_gate, w_up, w_down)


def solution(mesh):
    experts, groups = mesh.shape["expert"], mesh.shape["dp"]

    def shards(tokens, expert_ids, slots, mix_weights, w_gate, w_up, w_down):
        rows = experts * (groups // PLANE) * CAP
        fits = (
            groups % PLANE == 0
            and rows == 16
            and groups == 4 * PLANE
            and tokens.shape[0] == 8
            and experts * CAP <= 8
            and tokens.shape[1] % (HALVES * (rows // CAP) * 128) == 0
            and w_gate.shape[2] % (128 * PARTS) == 0
            and w_down.shape[2] % 128 == 0
        )
        form = kernel_form if fits else collective_form
        return form(tokens, expert_ids, slots, mix_weights, w_gate, w_up, w_down)

    placed = (
        P(("expert", "dp"), None),
        P(("expert", "dp"), None),
        P(("expert", "dp"), None),
        P(("expert", "dp"), None),
        P("expert", None, "dp"),
        P("expert", None, "dp"),
        P("expert", None, "dp"),
    )
    return jax.shard_map(
        shards, mesh=mesh, in_specs=placed, out_specs=P(("expert", "dp"), None), check_vma=False
    )
```
